32 devices in a mesh: grp: 2 (over y), seq: 4 (over z), head: 2 (over x), rep: 2 (over core).
Axes of the slice: x: 2, y: 2, z: 4, core: 2. Of those that a mesh axis runs over, the one named last changes fastest.
Arguments:
- queries: bfloat16 [32, 64, 128], P(('grp', 'rep'), 'head'), parts along dimension 0, may hold values from -16 to 16
- key_cache: bfloat16 [32, 4, 2048, 128], P(('grp', 'rep'), 'head', 'seq'), parts along dimension 0, may hold values from -7 to 7
- value_cache: bfloat16 [32, 4, 2048, 128], P(('grp', 'rep'), 'head', 'seq'), parts along dimension 0, may hold values from -6 to 6
- indices: int32 [32, 4, 16], P(('grp', 'rep'), 'head'), parts along dimension 0, may hold values from 0 to 31, as said below
- counts: int32 [32, 4], P(('grp', 'rep'), 'head'), parts along dimension 0, may hold values from 8 to 16, as said below
- lengths: int32 [32], P(('grp', 'rep')), parts along dimension 0, may hold values from 1024 to 2048
Outputs:
- attended: bfloat16 [32, 64, 128], P(('grp', 'rep'), 'head', 'seq'), parts along dimension 0
The draws below stay inside these ranges and needn't reach their ends.
There are 2 independent parts, one for each index of `grp`. The reference program is written for one: setup_inputs(seed, part) draws one part's arguments, and reference() takes and returns one part's arrays. A program takes and returns all parts, laid end to end along the dimension named above; each array names one. Nothing has to cross between parts.
Inputs may be any that keep to these rules, and one draw needn't show every extreme that they name: `indices`: within a row and key-value head the 16 blocks are distinct, and each holds at least one token below the row's length. `counts`: some row uses all 16 slots.
All inputs are finite; a program needn't handle non-finite values.
Results may differ from the reference program's by a relative error of at most 0.0015.
Values sent between devices are 32-bit elements; how exact they have to be, the bound alone decides.
No kernel may reach another device: no remote copies, remote signals or barrier semaphores. Data moves between devices by JAX's collectives and lax.ppermute only.
A program may use at most 64 MiB of HBM per device.

```python
import jax
import jax.numpy as jnp
from jax import lax

HEADS = 64
KVH = 4
DK = 128
DV = 128
BLOCK = 64
SLOTS = 16
BATCH = 16
CONTEXT = 2048


def selection(key):
    lengths = jax.random.randint(jax.random.fold_in(key, 11), (BATCH,), CONTEXT // 2, CONTEXT + 1)
    counts = jax.random.randint(jax.random.fold_in(key, 12), (BATCH, KVH), SLOTS // 2, SLOTS + 1)
    counts = jnp.where(jnp.arange(BATCH)[:, None] == 0, SLOTS, counts)
    blocks = CONTEXT // BLOCK
    finals = (lengths - 1) // BLOCK
    noise = jax.random.randint(jax.random.fold_in(key, 13), (BATCH, KVH, blocks), 0, 1 << 16)
    numbers = jnp.arange(blocks)
    noise = noise * blocks + numbers[None, None, :]
    inside = (numbers[None, None, :] >= 1) & (numbers[None, None, :] < finals[:, None, None])
    ranked = jnp.where(inside, noise, noise + (1 << 16) * blocks)
    order = jnp.argsort(ranked, axis=-1, stable=True)[:, :, :SLOTS - 2]
    first = jnp.zeros((BATCH, KVH, 1), jnp.int32)
    latest = jnp.broadcast_to(finals[:, None, None], (BATCH, KVH, 1))
    indices = jnp.concatenate([first, latest.astype(jnp.int32), order.astype(jnp.int32)], axis=-1)
    return (lengths.astype(jnp.int32), counts.astype(jnp.int32), indices)


def draw_indices(key, part):
    return selection(key)[2]


def draw_counts(key, part):
    return selection(key)[1]


def draw_lengths(key, part):
    return selection(key)[0]


def draw_queries(key, part):
    base = jnp.clip(4.0 * jax.random.normal(jax.random.fold_in(key, 3), (BATCH, HEADS, DK), jnp.float32), -16.0, 16.0)
    return base.astype(jnp.bfloat16)


def draw_key_cache(key, part):
    base = jnp.clip(jax.random.normal(jax.random.fold_in(key, 5), (BATCH, KVH, CONTEXT, DK), jnp.float32), -7.0, 7.0)
    return base.astype(jnp.bfloat16)


def steps_of(own_key, extent, split, smallest, high):
    gain = 1.0
    for dim, shards_of in split:
        heights = jax.random.uniform(jax.random.fold_in(jax.random.fold_in(own_key, 6), dim), (shards_of,), jnp.float32, smallest / len(split), high / len(split))
        gain = gain * jnp.repeat(jnp.exp(heights), extent[dim] // shards_of).reshape((-1,) + (1,) * (len(extent) - 1 - dim))
    return gain


def gaussian(key, dims, width, most, cuts=(), kind=jnp.bfloat16):
    result = width * jax.random.normal(key, dims, jnp.float32)
    if cuts:
        result = result * steps_of(key, dims, cuts, -0.22, 0.18)
    return jnp.clip(result, -most, most).astype(kind)


def setup_inputs(seed: int = 0, part: int = 0) -> dict:
    seeds = jax.random.split(jax.random.key(seed), 7)
    part_keys = jax.random.split(jax.random.fold_in(seeds[6], part), 7)
    return {
        "queries": draw_queries(jax.random.fold_in(jax.random.fold_in(seeds[6], part), 71), part),
        "key_cache": draw_key_cache(jax.random.fold_in(jax.random.fold_in(seeds[6], part), 71), part),
        "value_cache": gaussian(part_keys[2], (BATCH, KVH, CONTEXT, DV), 1.0, 6.0, ((0, 2), (1, 2), (2, 4))),
        "indices": draw_indices(jax.random.fold_in(jax.random.fold_in(seeds[6], part), 71), part),
        "counts": draw_counts(jax.random.fold_in(jax.random.fold_in(seeds[6], part), 71), part),
        "lengths": draw_lengths(jax.random.fold_in(jax.random.fold_in(seeds[6], part), 71), part),
    }


def attend_row(packed):
    query_row, key_row, value_row, index_row, count_row, length_row = packed
    group = HEADS // KVH
    rescale_factor = DK ** -0.5
    query_grouped = query_row.reshape(KVH, group, DK).astype(jnp.float32)
    key_blocks = key_row.reshape(KVH, CONTEXT // BLOCK, BLOCK, DK)
    value_blocks = value_row.reshape(KVH, CONTEXT // BLOCK, BLOCK, DV)
    chosen = index_row.astype(jnp.int32)
    chosen_keys = jnp.take_along_axis(key_blocks, chosen[:, :, None, None], axis=1)
    chosen_keys = chosen_keys.reshape(KVH, SLOTS * BLOCK, DK).astype(jnp.float32)
    picked_value_rows = jnp.take_along_axis(value_blocks, chosen[:, :, None, None], axis=1)
    picked_value_rows = picked_value_rows.reshape(KVH, SLOTS * BLOCK, DV).astype(jnp.float32)
    offsets = jnp.arange(BLOCK, dtype=jnp.int32)
    position = chosen[:, :, None] * BLOCK + offsets[None, None, :]
    used = jnp.arange(SLOTS, dtype=jnp.int32)[None, :, None] < count_row[:, None, None]
    live = (used & (position < length_row)).reshape(KVH, SLOTS * BLOCK)
    scores = jnp.einsum("hgd,hkd->hgk", query_grouped, chosen_keys, precision=lax.Precision.HIGHEST) * rescale_factor
    scores = jnp.where(live[:, None, :], scores, -jnp.inf)
    highest = jnp.max(scores, axis=-1, keepdims=True)
    softmax_weights = jnp.exp(scores - highest)
    total = jnp.sum(softmax_weights, axis=-1)
    weighted_value_sum = jnp.einsum("xcd,xdr->xcr", softmax_weights, picked_value_rows, precision=lax.Precision.HIGHEST)
    return (weighted_value_sum / total[..., None]).reshape(HEADS, DV).astype(jnp.bfloat16)


def reference(queries, key_cache, value_cache, indices, counts, lengths):
    return lax.map(attend_row, (queries, key_cache, value_cache, indices, counts, lengths))
```

```python
import functools

import jax
import jax.numpy as jnp
from jax import lax
from jax.experimental import pallas as pl
from jax.experimental.pallas import tpu as pltpu
from jax.sharding import PartitionSpec as P

BLOCK = 64
LANES = 128
SUBLANES = 8
LOG2E = 1.4426950408889634

lowest = -1e30
masked = -2e30


def partial_kernel(
    seq_count,
    relative,
    queries_hbm,
    keys_hbm,
    values_hbm,
    indices_hbm,
    counts_hbm,
    lengths_hbm,
    *refs,
):
    outs = refs[: seq_count if relative else 1]
    (
        queries,
        keys,
        values,
        indices,
        counts,
        lengths,
        weights,
        summed,
        flipped,
        small_sems,
        key_sems,
        value_sems,
    ) = refs[len(outs) :]
    batch_rows, heads_local, ctx_local, key_width = keys_hbm.shape
    value_width = values_hbm.shape[3]
    group = queries_hbm.shape[1] // heads_local
    slots = indices_hbm.shape[2]
    pairs = [(b, h) for b in range(batch_rows) for h in range(heads_local)]
    share = value_width // seq_count
    seq_index = lax.axis_index("seq")

    small = [
        pltpu.make_async_copy(src, dst, small_sems.at[n])
        for n, (src, dst) in enumerate(
            (
                (indices_hbm, indices),
                (counts_hbm, counts),
                (lengths_hbm, lengths),
                (queries_hbm, queries),
            )
        )
    ]
    for copy in small:
        copy.start()
    key_copies = [
        pltpu.make_async_copy(keys_hbm.at[b, h], keys.at[n], key_sems.at[n])
        for n, (b, h) in enumerate(pairs)
    ]
    value_copies = [
        pltpu.make_async_copy(values_hbm.at[b, h], values.at[n], value_sems.at[n])
        for n, (b, h) in enumerate(pairs)
    ]
    for copy in key_copies:
        copy.start()
    for copy in value_copies:
        copy.start()
    for copy in small:
        copy.wait()

    blocks = ctx_local // BLOCK
    base = seq_index * blocks
    slot = lax.broadcasted_iota(jnp.int32, (1, slots), 1)
    lane = lax.broadcasted_iota(jnp.int32, (1, ctx_local), 1)
    lane_block = lane // BLOCK
    position = lane + seq_index * ctx_local
    scale = LOG2E * key_width ** (-0.5)

    per_tile = LANES // group
    tiles = len(pairs) // per_tile
    row = lax.broadcasted_iota(jnp.int32, (group, LANES), 0)
    column = lax.broadcasted_iota(jnp.int32, (group, LANES), 1)
    tops = [jnp.zeros((group, LANES), jnp.float32) for _ in range(tiles)]
    totals = [jnp.zeros((group, LANES), jnp.float32) for _ in range(tiles)]
    for n, (b, h) in enumerate(pairs):
        offset = indices[b, h : h + 1, :] - base
        used = (slot < counts[h, b]) & (offset >= 0) & (offset < blocks)
        bits = jnp.sum(jnp.where(used, 1 << (offset & 31), 0), axis=1, keepdims=True)
        live = (((bits >> lane_block) & 1) != 0) & (position < lengths[b])
        key_copies[n].wait()
        scores = lax.dot_general(
            queries[b, h * group : (h + 1) * group, :],
            keys[n],
            (((1,), (1,)), ((), ())),
            preferred_element_type=jnp.float32,
        )
        scores = jnp.where(live, scores * scale, masked)
        top = jnp.maximum(jnp.max(scores, axis=1, keepdims=True), lowest)
        softmax_weights = jnp.exp2(scores - top)
        total = jnp.sum(softmax_weights, axis=1, keepdims=True)
        high = softmax_weights.astype(jnp.bfloat16)
        low = (softmax_weights - high.astype(jnp.float32)).astype(jnp.bfloat16)
        weights[n, :group] = high
        weights[n, group:] = low
        tile = n // per_tile
        mine = column == row + (n % per_tile) * group
        tops[tile] = jnp.where(mine, top, tops[tile])
        totals[tile] = jnp.where(mine, total, totals[tile])
    for n in range(len(pairs)):
        value_copies[n].wait()
        both = lax.dot_general(
            weights[n],
            values[n],
            (((1,), (0,)), ((), ())),
            preferred_element_type=jnp.float32,
        )
        summed[n * group : (n + 1) * group, :] = both[:group] + both[group:]

    stats = jnp.zeros((SUBLANES, LANES), jnp.float32)
    line = lax.broadcasted_iota(jnp.int32, (SUBLANES, LANES), 0)
    for tile in range(tiles):
        stats = jnp.where(line == tile, jnp.sum(tops[tile], axis=0, keepdims=True), stats)
        stats = jnp.where(line == tiles + tile, jnp.sum(totals[tile], axis=0, keepdims=True), stats)
        flipped[tile] = summed[tile * LANES : (tile + 1) * LANES, :].T

    for s in range(seq_count):
        if relative:
            out = outs[s]
            start = pl.multiple_of((seq_index ^ s) * share, share)
            for tile in range(tiles):
                out[tile * share : (tile + 1) * share] = flipped[tile, pl.ds(start, share), :]
            out[tiles * share :] = stats
        else:
            for tile in range(tiles):
                outs[0][s, tile * share : (tile + 1) * share] = flipped[
                    tile, s * share : (s + 1) * share, :
                ]
            outs[0][s, outs[0].shape[1] - SUBLANES :] = stats


def join_kernel(tiles, share, group, *refs):
    *pieces, out = refs
    if len(pieces) == 1:
        pieces = [pieces[0].at[s] for s in range(pieces[0].shape[0])]
    stats = [piece[piece.shape[0] - SUBLANES :] for piece in pieces]
    batch_rows = out.shape[0]
    per_row = out.shape[1]
    rows_of_tile = LANES // per_row
    for tile in range(tiles):
        tops = [stat[tile : tile + 1] for stat in stats]
        highest = functools.reduce(jnp.maximum, tops)
        factors = [jnp.exp2(top - highest) for top in tops]
        total = sum(
            factor * stat[tiles + tile : tiles + tile + 1]
            for factor, stat in zip(factors, stats, strict=True)
        )
        weighted = sum(
            factor * piece[tile * share : (tile + 1) * share]
            for factor, piece in zip(factors, pieces, strict=True)
        )
        result = (weighted / total).T
        out[tile * rows_of_tile : (tile + 1) * rows_of_tile] = result.reshape(
            rows_of_tile, per_row, share
        ).astype(out.dtype)


def local(queries, key_cache, value_cache, indices, counts, lengths):
    batch_rows, heads_local, ctx_local, key_width = key_cache.shape
    value_width = value_cache.shape[3]
    heads = queries.shape[1]
    group = heads // heads_local
    seq_count = lax.axis_size("seq")
    share = value_width // seq_count
    pairs = batch_rows * heads_local
    tiles = pairs * group // LANES
    piece_rows = -(-tiles * share // SUBLANES) * SUBLANES + SUBLANES
    relative = seq_count in (2, 4, 8)
    any_space = pl.BlockSpec(memory_space=pltpu.HBM)
    vmem = pl.BlockSpec(memory_space=pltpu.VMEM)
    if relative:
        out_shape = [jax.ShapeDtypeStruct((piece_rows, LANES), jnp.float32)] * seq_count
    else:
        out_shape = [jax.ShapeDtypeStruct((seq_count, piece_rows, LANES), jnp.float32)]
    pieces = pl.pallas_call(
        functools.partial(partial_kernel, seq_count, relative),
        out_shape=out_shape,
        in_specs=[any_space] * 6,
        out_specs=[vmem] * len(out_shape),
        scratch_shapes=[
            pltpu.VMEM(queries.shape, queries.dtype),
            pltpu.VMEM((pairs, ctx_local, key_width), key_cache.dtype),
            pltpu.VMEM((pairs, ctx_local, value_width), value_cache.dtype),
            pltpu.VMEM(indices.shape, indices.dtype),
            pltpu.SMEM((heads_local, batch_rows), counts.dtype),
            pltpu.SMEM(lengths.shape, lengths.dtype),
            pltpu.VMEM((pairs, 2 * group, ctx_local), jnp.bfloat16),
            pltpu.VMEM((pairs * group, value_width), jnp.float32),
            pltpu.VMEM((tiles, value_width, LANES), jnp.float32),
            pltpu.SemaphoreType.DMA((4,)),
            pltpu.SemaphoreType.DMA((pairs,)),
            pltpu.SemaphoreType.DMA((pairs,)),
        ],
        name="partial_attention",
    )(queries, key_cache, value_cache, indices, counts.T, lengths)
    if relative:
        arrived = [pieces[0]] + [
            lax.ppermute(pieces[s], "seq", [(i, i ^ s) for i in range(seq_count)])
            for s in range(seq_count - 1, 0, -1)
        ]
    else:
        arrived = [lax.all_to_all(pieces[0], "seq", 0, 0)]
    return pl.pallas_call(
        functools.partial(join_kernel, tiles, share, group),
        out_shape=jax.ShapeDtypeStruct((batch_rows, heads, share), jnp.bfloat16),
        in_specs=[vmem] * len(arrived),
        out_specs=vmem,
        name="join_partials",
    )(*arrived)


def solution(mesh):
    return jax.shard_map(
        local,
        mesh=mesh,
        in_specs=(
            P(("grp", "rep"), "head", None),
            P(("grp", "rep"), "head", "seq", None),
            P(("grp", "rep"), "head", "seq", None),
            P(("grp", "rep"), "head", None),
            P(("grp", "rep"), "head"),
            P(("grp", "rep")),
        ),
        out_specs=P(("grp", "rep"), "head", "seq"),
        check_vma=False,
    )
```

```python
import functools

import jax
import jax.numpy as jnp
from jax import lax
from jax.experimental import pallas as pl
from jax.experimental.pallas import tpu as pltpu
from jax.sharding import PartitionSpec as P

BLOCK = 64
LANES = 128
SUBLANES = 8
CHUNKS = 1
LAG = 1
LOG2E = 1.4426950408889634

lowest = -1e30
masked = -2e30


def partial_kernel(
    seq_count,
    relative,
    queries_hbm,
    keys_hbm,
    values_hbm,
    indices_hbm,
    counts_hbm,
    lengths_hbm,
    *refs,
):
    outs = refs[: seq_count if relative else 1]
    (
        queries,
        keys,
        values,
        indices,
        counts,
        lengths,
        flipped,
        small_sems,
        key_sems,
        value_sems,
    ) = refs[len(outs) :]
    batch_rows, heads_local, ctx_local, key_width = keys_hbm.shape
    value_width = values_hbm.shape[3]
    group = queries_hbm.shape[1] // heads_local
    slots = indices_hbm.shape[2]
    share = value_width // seq_count
    chunks = key_sems.shape[0]
    rows = batch_rows // chunks
    seq_index = lax.axis_index("seq")

    small = [
        pltpu.make_async_copy(src, dst, small_sems.at[n])
        for n, (src, dst) in enumerate(
            (
                (indices_hbm, indices),
                (counts_hbm, counts),
                (lengths_hbm, lengths),
                (queries_hbm, queries),
            )
        )
    ]

    def pieces_of(chunk, src, dst, sems):
        return [
            pltpu.make_async_copy(src.at[b, h], dst.at[b, h], sems.at[chunk])
            for b in range(chunk * rows, (chunk + 1) * rows)
            for h in range(heads_local)
        ]

    def whole_of(chunk, src, dst, sems):
        part = pl.ds(chunk * rows, rows)
        return pltpu.make_async_copy(src.at[part], dst.at[part], sems.at[chunk])

    key_side = (keys_hbm, keys, key_sems)
    value_side = (values_hbm, values, value_sems)
    for copy in small:
        copy.start()
    for step in range(chunks + LAG):
        if step < chunks:
            for copy in pieces_of(step, *key_side):
                copy.start()
        if step >= LAG:
            for copy in pieces_of(step - LAG, *value_side):
                copy.start()
    for copy in small:
        copy.wait()

    blocks = ctx_local // BLOCK
    base = seq_index * blocks
    slot = lax.broadcasted_iota(jnp.int32, (1, slots), 1)
    lane = lax.broadcasted_iota(jnp.int32, (1, ctx_local), 1)
    lane_block = lane // BLOCK
    position = lane + seq_index * ctx_local
    scale = LOG2E * key_width ** (-0.5)

    def live_of(b, h):
        offset = indices[b, h : h + 1, :] - base
        used = (slot < counts[h, b]) & (offset >= 0) & (offset < blocks)
        bits = jnp.sum(jnp.where(used, 1 << (offset & 31), 0), axis=1, keepdims=True)
        return (((bits >> lane_block) & 1) != 0) & (position < lengths[b])

    def scores_of(b, h):
        return lax.dot_general(
            queries[b, h * group : (h + 1) * group, :],
            keys[b, h],
            (((1,), (1,)), ((), ())),
            preferred_element_type=jnp.float32,
        )

    def weights_of(scores, live):
        scores = jnp.where(live, scores * scale, masked)
        top = jnp.maximum(jnp.max(scores, axis=1, keepdims=True), lowest)
        softmax_weights = jnp.exp2(scores - top)
        total = jnp.sum(softmax_weights, axis=1, keepdims=True)
        high = softmax_weights.astype(jnp.bfloat16)
        low = (softmax_weights - high.astype(jnp.float32)).astype(jnp.bfloat16)
        return jnp.concatenate([high, low], axis=0), top, total

    def summed_of(b, h, weights):
        both = jnp.dot(weights, values[b, h], preferred_element_type=jnp.float32)
        return both[:group] + both[group:]

    per_tile = LANES // group
    pairs = [(b, h) for b in range(batch_rows) for h in range(heads_local)]
    tiles = len(pairs) // per_tile
    row = lax.broadcasted_iota(jnp.int32, (group, LANES), 0)
    column = lax.broadcasted_iota(jnp.int32, (group, LANES), 1)
    tops = [jnp.zeros((group, LANES), jnp.float32) for _ in range(tiles)]
    totals = [jnp.zeros((group, LANES), jnp.float32) for _ in range(tiles)]

    def chunk_pairs(chunk):
        size = rows * heads_local
        return list(enumerate(pairs))[chunk * size : (chunk + 1) * size]

    lives = [live_of(b, h) for b, h in pairs]
    scores, weights, summed = {}, {}, {}
    done_tiles = 0
    for step in range(chunks + 2):
        if step < chunks:
            whole_of(step, *key_side).wait()
        if step >= 2:
            whole_of(step - 2, *value_side).wait()
        if step < chunks:
            for n, (b, h) in chunk_pairs(step):
                scores[n] = scores_of(b, h)
        if 1 <= step <= chunks:
            for n, _ in chunk_pairs(step - 1):
                weights[n], top, total = weights_of(scores.pop(n), lives[n])
                tile = n // per_tile
                mine = column == row + (n % per_tile) * group
                tops[tile] = jnp.where(mine, top, tops[tile])
                totals[tile] = jnp.where(mine, total, totals[tile])
        if step >= 2:
            for n, (b, h) in chunk_pairs(step - 2):
                summed[n] = summed_of(b, h, weights.pop(n))
        while all(done_tiles * per_tile + n in summed for n in range(per_tile)):
            flipped[done_tiles] = jnp.concatenate(
                [summed.pop(done_tiles * per_tile + n) for n in range(per_tile)], axis=0
            ).T
            done_tiles += 1

    stats = jnp.zeros((SUBLANES, LANES), jnp.float32)
    line = lax.broadcasted_iota(jnp.int32, (SUBLANES, LANES), 0)
    for tile in range(tiles):
        stats = jnp.where(line == tile, jnp.sum(tops[tile], axis=0, keepdims=True), stats)
        stats = jnp.where(line == tiles + tile, jnp.sum(totals[tile], axis=0, keepdims=True), stats)

    for s in range(seq_count):
        if relative:
            out = outs[s]
            start = pl.multiple_of((seq_index ^ s) * share, share)
            for tile in range(tiles):
                out[tile * share : (tile + 1) * share] = flipped[tile, pl.ds(start, share), :]
            out[tiles * share :] = stats
        else:
            for tile in range(tiles):
                outs[0][s, tile * share : (tile + 1) * share] = flipped[
                    tile, s * share : (s + 1) * share, :
                ]
            outs[0][s, outs[0].shape[1] - SUBLANES :] = stats


def join_kernel(tiles, share, group, *refs):
    *pieces, out = refs
    if len(pieces) == 1:
        pieces = [pieces[0].at[s] for s in range(pieces[0].shape[0])]
    stats = [piece[piece.shape[0] - SUBLANES :] for piece in pieces]
    batch_rows = out.shape[0]
    per_row = out.shape[1]
    rows_of_tile = LANES // per_row
    for tile in range(tiles):
        tops = [stat[tile : tile + 1] for stat in stats]
        highest = functools.reduce(jnp.maximum, tops)
        factors = [jnp.exp2(top - highest) for top in tops]
        total = sum(
            factor * stat[tiles + tile : tiles + tile + 1]
            for factor, stat in zip(factors, stats, strict=True)
        )
        weighted = sum(
            factor * piece[tile * share : (tile + 1) * share]
            for factor, piece in zip(factors, pieces, strict=True)
        )
        result = (weighted / total).T
        out[tile * rows_of_tile : (tile + 1) * rows_of_tile] = result.reshape(
            rows_of_tile, per_row, share
        ).astype(out.dtype)


def local(queries, key_cache, value_cache, indices, counts, lengths):
    batch_rows, heads_local, ctx_local, key_width = key_cache.shape
    value_width = value_cache.shape[3]
    heads = queries.shape[1]
    group = heads // heads_local
    seq_count = lax.axis_size("seq")
    share = value_width // seq_count
    pairs = batch_rows * heads_local
    tiles = pairs * group // LANES
    piece_rows = -(-tiles * share // SUBLANES) * SUBLANES + SUBLANES
    relative = seq_count in (2, 4, 8)
    any_space = pl.BlockSpec(memory_space=pltpu.HBM)
    vmem = pl.BlockSpec(memory_space=pltpu.VMEM)
    if relative:
        out_shape = [pltpu.VMEM((piece_rows, LANES), jnp.float32)] * seq_count
    else:
        out_shape = [pltpu.VMEM((seq_count, piece_rows, LANES), jnp.float32)]
    pieces = pl.pallas_call(
        functools.partial(partial_kernel, seq_count, relative),
        out_shape=out_shape,
        in_specs=[any_space] * 6,
        out_specs=[vmem] * len(out_shape),
        scratch_shapes=[
            pltpu.VMEM(queries.shape, queries.dtype),
            pltpu.VMEM(key_cache.shape, key_cache.dtype),
            pltpu.VMEM(value_cache.shape, value_cache.dtype),
            pltpu.VMEM(indices.shape, indices.dtype),
            pltpu.SMEM((heads_local, batch_rows), counts.dtype),
            pltpu.SMEM(lengths.shape, lengths.dtype),
            pltpu.VMEM((tiles, value_width, LANES), jnp.float32),
            pltpu.SemaphoreType.DMA((4,)),
            pltpu.SemaphoreType.DMA((CHUNKS,)),
            pltpu.SemaphoreType.DMA((CHUNKS,)),
        ],
        compiler_params=pltpu.CompilerParams(vmem_limit_bytes=12 << 20),
        name="partial_attention",
    )(
        *(
            pltpu.with_memory_space_constraint(operand, pltpu.HBM)
            for operand in (queries, key_cache, value_cache, indices, counts.T, lengths)
        )
    )
    if relative:
        arrived = [pieces[0]] + [
            lax.ppermute(pieces[s], "seq", [(i, i ^ s) for i in range(seq_count)])
            for s in range(seq_count - 1, 0, -1)
        ]
    else:
        arrived = [lax.all_to_all(pieces[0], "seq", 0, 0)]
    return pl.pallas_call(
        functools.partial(join_kernel, tiles, share, group),
        out_shape=jax.ShapeDtypeStruct((batch_rows, heads, share), jnp.bfloat16),
        in_specs=[vmem] * len(arrived),
        out_specs=vmem,
        compiler_params=pltpu.CompilerParams(vmem_limit_bytes=4 << 20),
        name="join_partials",
    )(*arrived)


def solution(mesh):
    return jax.shard_map(
        local,
        mesh=mesh,
        in_specs=(
            P(("grp", "rep"), "head", None),
            P(("grp", "rep"), "head", "seq", None),
            P(("grp", "rep"), "head", "seq", None),
            P(("grp", "rep"), "head", None),
            P(("grp", "rep"), "head"),
            P(("grp", "rep")),
        ),
        out_specs=P(("grp", "rep"), "head", "seq"),
        check_vma=False,
    )
```
